32 devices in a mesh: gx: 4 (over y, core), gy: 4 (over z), gz: 2 (over x).
Axes of the slice: x: 2, y: 2, z: 4, core: 2. Of those that a mesh axis runs over, the one named last changes fastest.
Arguments:
- stream: bfloat16 [8192, 8192], P(('gx', 'gy', 'gz')), may hold values from -4 to 4
- segment_ids: int32 [8192], P(('gx', 'gy', 'gz')), may hold values from 0 to 8191, as said below
- positions: int32 [8192], P(('gx', 'gy', 'gz')), may hold values from 0 to 255, as said below
- norm_gain: bfloat16 [1, 8192], P(None, ('gx', 'gy', 'gz')), may hold values from 0.099609375 to 1.8984375
- q_weight: bfloat16 [1, 8192, 512], P(None, ('gx', 'gy', 'gz')), as said below
- k_weight: bfloat16 [1, 8192, 128], P(None, ('gx', 'gy', 'gz')), as said below
- v_weight: bfloat16 [1, 8192, 128], P(None, ('gx', 'gy', 'gz')), may hold values from -0.0625 to 0.0625
- o_weight: bfloat16 [1, 512, 8192], P(None, None, ('gx', 'gy', 'gz')), may hold values from -0.25 to 0.25
Outputs:
- result: bfloat16 [8192, 8192], P(('gx', 'gy', 'gz'))
The draws below stay inside these ranges and needn't reach their ends.
Inputs may be any that keep to these rules, and one draw needn't show every extreme that they name: `segment_ids`: each token's id is the index of its document's first token, so ids never fall along the tokens; every document lies inside one aligned block of 256 tokens, every block starts a new document, and the last token is a document of its own. `positions`: counts from 0 at a document's first token and rises by one per token. `q_weight`: A projection scaled by its fan-in. `k_weight`: A projection scaled by its fan-in.
All inputs are finite; a program needn't handle non-finite values.
Results may differ from the reference program's by a relative error of at most 0.0064.
Values may be sent and summed in bfloat16 or wider, within the bound.
A program may use at most 128 MiB of HBM per device.

```python
import math
import jax
import jax.numpy as jnp
from jax import lax

D = 8192
HD = 128
QH = 4
LAYERS = 1
TOK_DEV = 256
TOKENS = 8192


def segment_plan(key):
    base = jax.random.fold_in(key, 301)
    marks = jax.random.randint(base, (TOKENS,), 0, 80)
    index = jnp.arange(TOKENS, dtype=jnp.int32)
    starts = (marks == 0) | (index % TOK_DEV == 0) | (index == TOKENS - 1)
    begin = lax.cummax(jnp.where(starts, index, 0), axis=0)
    return (begin.astype(jnp.int32), (index - begin).astype(jnp.int32))


def draw_segment_ids(key, part):
    return segment_plan(key)[0]


def draw_positions(key, part):
    return segment_plan(key)[1]


def row_scales(key):
    return jnp.exp(jax.random.uniform(jax.random.fold_in(key, 411), (LAYERS, D, 1), jnp.float32, -0.7, 0.7))


def key_plan(key):
    noise_key = jax.random.fold_in(key, 401)
    base = jax.random.normal(noise_key, (LAYERS, D, HD), jnp.float32) * D ** (-0.5) * row_scales(key)
    return base


def draw_k_weight(key, part):
    return key_plan(key).astype(jnp.bfloat16)


def draw_q_weight(key, part):
    noise = jax.random.normal(jax.random.fold_in(key, 421), (LAYERS, D, QH * HD), jnp.float32) * D ** (-0.5) * row_scales(key)
    return noise.astype(jnp.bfloat16)


def levels(own_key, shape, shards, smallest, high):
    factor_of = 1.0
    for position, parts in shards:
        draws = jax.random.uniform(jax.random.fold_in(jax.random.fold_in(own_key, 6), position), (parts,), jnp.float32, smallest / len(shards), high / len(shards))
        factor_of = factor_of * jnp.repeat(jnp.exp(draws), shape[position] // parts).reshape((-1,) + (1,) * (len(shape) - 1 - position))
    return factor_of


def gaussian(rng, shape, scale, bound, pieces=(), held_as=jnp.bfloat16):
    factor_of = levels(rng, shape, pieces, -0.22, 0.18) if pieces else 1.0
    values = jax.random.normal(rng, shape, jnp.float32) * scale * factor_of
    return jnp.minimum(jnp.maximum(values, -bound), bound).astype(held_as)


def setup_inputs(seed: int = 0) -> dict:
    key_list = jax.random.split(jax.random.key(seed), 9)
    stream = gaussian(key_list[0], (TOKENS, D), 0.5, 4.0, ((0, 32),))
    segment_ids = draw_segment_ids(jax.random.fold_in(key_list[8], 71), 0)
    positions = draw_positions(jax.random.fold_in(key_list[8], 71), 0)
    norm_gain = jnp.clip(1.0 + 0.18 * jax.random.normal(key_list[3], (LAYERS, D), jnp.float32), 0.099609375, 1.8984375).astype(jnp.bfloat16)
    q_weight = draw_q_weight(jax.random.fold_in(key_list[8], 71), 0)
    k_weight = draw_k_weight(jax.random.fold_in(key_list[8], 71), 0)
    v_weight = gaussian(key_list[6], (LAYERS, D, HD), D ** -0.5, 0.0625, ((1, 32),))
    o_weight = gaussian(key_list[7], (LAYERS, QH * HD, D), (QH * HD) ** -0.5, 0.25, ((2, 32),))
    return {"stream": stream, "segment_ids": segment_ids, "positions": positions, "norm_gain": norm_gain, "q_weight": q_weight, "k_weight": k_weight, "v_weight": v_weight, "o_weight": o_weight}


def rotate(values, positions):
    width = values.shape[-1]
    half = width // 2
    freqs = jnp.exp(-math.log(500000.0) * jnp.arange(half, dtype=jnp.float32) * 2.0 / width)
    angles = positions.astype(jnp.float32)[:, None] * freqs[None, :]
    cosine = jnp.concatenate([jnp.cos(angles), jnp.cos(angles)], -1)[:, None, :]
    sine = jnp.concatenate([jnp.sin(angles), jnp.sin(angles)], -1)[:, None, :]
    turned = jnp.concatenate([-values[..., half:], values[..., :half]], -1)
    return values * cosine + turned * sine

def attend(queries, keys, values, segment_ids, positions):
    count = queries.shape[0]
    scores = jnp.einsum('thd,sd->hts', queries.astype(jnp.float32), keys.astype(jnp.float32)) / math.sqrt(keys.shape[-1])
    allowed = (segment_ids[:, None] == segment_ids[None, :]) & (positions[None, :] <= positions[:, None])
    scores = jnp.where(allowed[None], scores, -1e+30)
    peak = lax.optimization_barrier(jnp.max(scores, -1, keepdims=True))
    expd = jnp.exp(scores - peak)
    probs = (expd / lax.optimization_barrier(jnp.sum(expd, -1, keepdims=True))).astype(jnp.bfloat16)
    mixed = jnp.einsum('hts,sd->thd', probs.astype(jnp.float32), values.astype(jnp.float32))
    return mixed.astype(jnp.bfloat16).reshape(count, -1)

def run_block(block, segment_ids, positions, norm_gain, q_weight, k_weight, v_weight, o_weight):
    count = block.shape[0]
    current = block
    for layer in range(LAYERS):
        widened = lax.optimization_barrier(current).astype(jnp.float32)
        inverse = lax.rsqrt(lax.optimization_barrier(jnp.mean(widened * widened, -1, keepdims=True)) + 1e-05)
        normed = (widened * inverse * norm_gain[layer].astype(jnp.float32)).astype(jnp.bfloat16)
        query_raw = jnp.dot(normed, q_weight[layer], preferred_element_type=jnp.float32)
        key_raw = jnp.dot(normed, k_weight[layer], preferred_element_type=jnp.float32)
        value_raw = jnp.dot(normed, v_weight[layer], preferred_element_type=jnp.float32)
        queries = rotate(query_raw.reshape(count, QH, HD), positions).astype(jnp.bfloat16)
        keys = rotate(key_raw[:, None, :], positions)[:, 0, :].astype(jnp.bfloat16)
        values = value_raw.astype(jnp.bfloat16)
        mixed = attend(queries, keys, values, segment_ids, positions)
        branch = jnp.dot(mixed, o_weight[layer], preferred_element_type=jnp.float32)
        current = (widened + branch).astype(jnp.bfloat16)
    return current

def reference(stream, segment_ids, positions, norm_gain, q_weight, k_weight, v_weight, o_weight):
    blocks = TOKENS // TOK_DEV

    def one(item):
        return run_block(item[0], item[1], item[2], norm_gain, q_weight, k_weight, v_weight, o_weight)
    result = lax.map(one, (stream.reshape(blocks, TOK_DEV, D), segment_ids.reshape(blocks, TOK_DEV), positions.reshape(blocks, TOK_DEV)), batch_size=8)
    return result.reshape(TOKENS, D)
```

```python
import functools
import itertools
import math

import jax
import jax.numpy as jnp
from jax import lax
from jax.experimental import pallas as pl
from jax.experimental.pallas import tpu as pltpu
from jax.sharding import PartitionSpec as P

AXES = ("gx", "gy", "gz")
CORES = 2
MAX_RECEIVES = 256
ORDERS = ((0, 1, 2), (1, 0, 2), (2, 0, 1), (2, 1, 0))
SHARES = (1, 1, 3, 3)


def rotate(values, positions):
    width = values.shape[-1]
    half = width // 2
    freqs = jnp.exp(-math.log(500000.0) * jnp.arange(half, dtype=jnp.float32) * 2.0 / width)
    angles = positions.astype(jnp.float32)[:, None] * freqs[None, :]
    cosine = jnp.concatenate([jnp.cos(angles), jnp.cos(angles)], -1)[:, None, :]
    sine = jnp.concatenate([jnp.sin(angles), jnp.sin(angles)], -1)[:, None, :]
    turned = jnp.concatenate([-values[..., half:], values[..., :half]], -1)
    return values * cosine + turned * sine


def attend(queries, keys, values, segment_ids, positions):
    count = queries.shape[0]
    scores = jnp.einsum(
        "thd,sd->hts", queries, keys, preferred_element_type=jnp.float32
    ) / math.sqrt(keys.shape[-1])
    allowed = (segment_ids[:, None] == segment_ids[None, :]) & (
        positions[None, :] <= positions[:, None]
    )
    scores = jnp.where(allowed[None], scores, -1e30)
    peak = jnp.max(scores, -1, keepdims=True)
    expd = jnp.exp(scores - peak)
    probs = (expd / jnp.sum(expd, -1, keepdims=True)).astype(jnp.bfloat16)
    mixed = jnp.einsum("hts,sd->thd", probs, values, preferred_element_type=jnp.float32)
    return mixed.astype(jnp.bfloat16).reshape(count, -1)


def arrivals(size):
    return [sorted(range(size), key=lambda other: (abs(other - own), other)) for own in range(size)]


def pick(table, place):
    if len(set(table)) == 1:
        return table[0]
    value = jnp.int32(table[0])
    for index in range(1, len(table)):
        value = jnp.where(place == index, jnp.int32(table[index]), value)
    return value


def pieces_of(rows, unit):
    units = rows // unit
    total = sum(SHARES)
    runs, start, seen = [], 0, 0
    for share in SHARES:
        seen += share
        stop = units * seen // total * unit
        runs.append((start, stop))
        start = stop
    return runs


def program_order(dims, pieces):
    events = []
    for number, (tensor, order, _) in enumerate(pieces):
        for combo in itertools.product(*(range(size) for size in dims)):
            hops, late = 0, 0
            for place, axis in enumerate(order):
                hops += combo[axis]
                late = late * 8 + combo[order[2 - place]]
            if hops:
                events.append((tensor, hops, late, number, combo))
    events.sort()
    return [(number, combo) for _, _, _, number, combo in events]


class Gather:
    def __init__(self, dims, pieces, refs_in, refs_out, slices, own_sems, send_sem, recv_sem, cross_sem):
        self.dims, self.pieces = dims, pieces
        self.refs_in, self.refs_out, self.slices = refs_in, refs_out, slices
        self.send_sem, self.recv_sem, self.cross_sem = send_sem, recv_sem, cross_sem
        gx, gy, gz = (lax.axis_index(name) for name in AXES)
        self.core = lax.rem(gx, CORES)
        self.me = (gz, lax.div(gx, CORES), gy)
        self.tables = [arrivals(size) for size in dims]
        self.sends = 0
        self.pending = []

    def device(self, place, core):
        x, y, z = place
        return (y * CORES + core, z, x)

    def line(self, place):
        x, y, z = place
        return (y * self.dims[2] + z) * self.dims[0] + x

    def block(self, place, core):
        x, y, z = place
        return ((y * CORES + core) * self.dims[2] + z) * self.dims[0] + x

    def neighbour(self, axis, step):
        place = list(self.me)
        place[axis] = place[axis] + step
        return tuple(place)

    def other(self, axis):
        place = list(self.me)
        place[axis] = 1 - place[axis]
        return tuple(place)

    def barrier(self):
        sem = pltpu.get_barrier_semaphore()
        mesh = pl.DeviceIdType.MESH
        count = 1
        pl.semaphore_signal(sem, inc=1, device_id=self.device(self.me, 1 - self.core), device_id_type=mesh)
        for axis, size in enumerate(self.dims):
            if size == 2:
                pl.semaphore_signal(
                    sem, inc=1, device_id=self.device(self.other(axis), self.core), device_id_type=mesh
                )
                count = count + 1
            elif size > 2:
                for step in (-1, 1):
                    inside = self.inside(axis, step)

                    @pl.when(inside)
                    def _(axis=axis, step=step):
                        pl.semaphore_signal(
                            sem,
                            inc=1,
                            device_id=self.device(self.neighbour(axis, step), self.core),
                            device_id_type=mesh,
                        )

                    count = count + inside.astype(jnp.int32)
        pl.semaphore_wait(sem, count)

    def inside(self, axis, step):
        return self.me[axis] > 0 if step < 0 else self.me[axis] < self.dims[axis] - 1

    def source(self, number, owner, own):
        tensor = self.pieces[number][0]
        if own:
            return self.slices[tensor](self.refs_in[tensor], None, self.pieces[number][2])
        return self.slices[tensor](self.refs_out[tensor], self.block(owner, self.core), self.pieces[number][2])

    def copy(self, number, owner, own, device, sem, cross=False):
        tensor = self.pieces[number][0]
        target = self.slices[tensor](self.refs_out[tensor], self.block(owner, self.core), self.pieces[number][2])
        landed = self.cross_sem if cross else self.recv_sem
        return pltpu.make_async_remote_copy(
            src_ref=self.source(number, owner, own),
            dst_ref=target,
            send_sem=self.send_sem.at[sem],
            recv_sem=landed.at[number, self.line(owner)],
            device_id=device,
            device_id_type=pl.DeviceIdType.MESH,
        )

    def send(self, number, owner, own, place, condition=None, cross=False):
        sem = self.sends
        self.sends += 1
        core = 1 - self.core if cross else self.core

        def make():
            return self.copy(number, owner, own, self.device(place, core), sem, cross)

        if condition is None:
            make().start()
        else:
            pl.when(condition)(lambda: make().start())
        self.pending.append((make, condition))

    def pass_on(self, number, combo):
        order = self.pieces[number][1]
        owner = tuple(
            pick([row[index] for row in table], here)
            for table, index, here in zip(self.tables, combo, self.me)
        )
        own = not any(combo)
        last = max((place for place, axis in enumerate(order) if combo[axis]), default=-1)
        if last >= 0:
            axis = order[last]
            if self.dims[axis] > 2:
                up = owner[axis] < self.me[axis]
                step = jnp.where(up, 1, -1)
                goes = jnp.where(up, self.me[axis] < self.dims[axis] - 1, self.me[axis] > 0)
                self.send(number, owner, own, self.neighbour(axis, step), goes)
        for axis in order[last + 1 :]:
            if self.dims[axis] == 2:
                self.send(number, owner, own, self.other(axis))
            elif self.dims[axis] > 2:
                for step in (-1, 1):
                    self.send(number, owner, own, self.neighbour(axis, step), self.inside(axis, step))
        self.send(number, owner, own, self.me, cross=True)

    def take(self, number, combo, cross=False):
        owner = tuple(
            pick([row[index] for row in table], here)
            for table, index, here in zip(self.tables, combo, self.me)
        )
        tensor = self.pieces[number][0]
        core = 1 - self.core if cross else self.core
        landed = self.slices[tensor](self.refs_out[tensor], self.block(owner, core), self.pieces[number][2])
        sem = self.cross_sem if cross else self.recv_sem
        pltpu.make_async_copy(landed, landed, sem.at[number, self.line(owner)]).wait()

    def drain(self):
        for make, condition in self.pending:
            if condition is None:
                make().wait_send()
            else:
                pl.when(condition)(lambda make=make: make().wait_send())


def gather_kernel(dims, pieces, order, w_ref, o_ref, wf_ref, of_ref, own_sem, send_sem, recv_sem, cross_sem):
    rows = w_ref.shape[0]
    cols = o_ref.shape[1]

    def w_slice(ref, block, run):
        start = run[0] if block is None else block * rows + run[0]
        if block is not None:
            start = pl.multiple_of(start, 16)
        return ref.at[pl.ds(start, run[1] - run[0]), :]

    def o_slice(ref, block, run):
        if block is None:
            return ref.at[pl.ds(run[0], run[1] - run[0]), :]
        return ref.at[pl.ds(run[0], run[1] - run[0]), pl.ds(pl.multiple_of(block * cols, cols), cols)]

    g = Gather(dims, pieces, (w_ref, o_ref), (wf_ref, of_ref), (w_slice, o_slice), own_sem, send_sem, recv_sem, cross_sem)
    mine = g.block(g.me, g.core)
    keep_w = pltpu.make_async_copy(w_ref, w_slice(wf_ref, mine, (0, rows)), own_sem.at[0])
    keep_o = pltpu.make_async_copy(o_ref, o_slice(of_ref, mine, (0, o_ref.shape[0])), own_sem.at[1])
    g.barrier()
    keep_w.start()
    keep_o.start()
    zero = (0, 0, 0)
    for number, piece in enumerate(pieces):
        if piece[0] == 0:
            g.pass_on(number, zero)
    weights = sum(1 for number, _ in order if pieces[number][0] == 0)
    for index, (number, combo) in enumerate(order):
        if index == weights // 2:
            for later, piece in enumerate(pieces):
                if piece[0] == 1:
                    g.pass_on(later, zero)
        g.take(number, combo)
        g.pass_on(number, combo)
    for number, combo in [(number, zero) for number in range(len(pieces))] + list(order):
        g.take(number, combo, cross=True)
    g.drain()
    keep_w.wait()
    keep_o.wait()


def count_sends(dims, pieces):
    total = 0
    for _, order, _ in pieces:
        for combo in itertools.product(*(range(size) for size in dims)):
            last = max((place for place, axis in enumerate(order) if combo[axis]), default=-1)
            if last >= 0 and dims[order[last]] > 2:
                total += 1
            total += sum(min(dims[axis] - 1, 2) for axis in order[last + 1 :]) + 1
    return total


def gather_all(dims, weight, out_weight):
    rows, width = weight.shape
    depth, cols = out_weight.shape
    count = math.prod(dims) * CORES
    pieces = [(0, order, run) for order, run in zip(ORDERS, pieces_of(rows, 16))]
    pieces += [(1, order, run) for order, run in zip(ORDERS, pieces_of(depth, 16))]
    pieces = [piece for piece in pieces if piece[2][1] > piece[2][0]]
    order = program_order(dims, pieces)
    lines = math.prod(dims)
    return pl.pallas_call(
        functools.partial(gather_kernel, dims, pieces, order),
        out_shape=(
            jax.ShapeDtypeStruct((count * rows, width), weight.dtype),
            jax.ShapeDtypeStruct((depth, count * cols), out_weight.dtype),
        ),
        in_specs=[pl.BlockSpec(memory_space=pl.ANY)] * 2,
        out_specs=[pl.BlockSpec(memory_space=pl.ANY)] * 2,
        scratch_shapes=[
            pltpu.SemaphoreType.DMA((2,)),
            pltpu.SemaphoreType.DMA((count_sends(dims, pieces),)),
            pltpu.SemaphoreType.DMA((len(pieces), lines)),
            pltpu.SemaphoreType.DMA((len(pieces), lines)),
        ],
        compiler_params=pltpu.CompilerParams(collective_id=0, has_side_effects=True),
    )(weight, out_weight)


def body(dims, stream, segment_ids, positions, norm_gain, q_weight, k_weight, v_weight, o_weight):
    count = stream.shape[0]
    head_size = k_weight.shape[2]
    queries_width = q_weight.shape[2]
    widened = stream.astype(jnp.float32)
    inverse = lax.rsqrt(jnp.mean(widened * widened, -1, keepdims=True) + 1e-05)
    joined = jnp.concatenate([q_weight[0], k_weight[0], v_weight[0]], -1).astype(jnp.float32)
    weight = (joined * norm_gain[0].astype(jnp.float32)[:, None]).astype(jnp.bfloat16)
    if CORES * len(ORDERS) * math.prod(dims) <= MAX_RECEIVES:
        full, out_full = gather_all(dims, weight, o_weight[0])
    else:
        full, out_full = weight, o_weight[0]
        for name in reversed(AXES):
            full = lax.all_gather(full, name, axis=0, tiled=True)
            out_full = lax.all_gather(out_full, name, axis=1, tiled=True)
    raw = jnp.dot(stream, full, preferred_element_type=jnp.float32) * inverse
    query_raw = raw[:, :queries_width]
    key_raw = raw[:, queries_width : queries_width + head_size]
    value_raw = raw[:, queries_width + head_size :]
    queries = rotate(query_raw.reshape(count, -1, head_size), positions).astype(jnp.bfloat16)
    keys = rotate(key_raw[:, None, :], positions)[:, 0, :].astype(jnp.bfloat16)
    values = value_raw.astype(jnp.bfloat16)
    mixed = attend(queries, keys, values, segment_ids, positions)
    branch = jnp.dot(mixed, out_full, preferred_element_type=jnp.float32)
    return (widened + branch).astype(jnp.bfloat16)


def solution(mesh):
    tokens = AXES
    in_specs = (
        P(tokens, None),
        P(tokens),
        P(tokens),
        P(None, tokens),
        P(None, tokens, None),
        P(None, tokens, None),
        P(None, tokens, None),
        P(None, None, tokens),
    )
    dims = (mesh.shape["gz"], mesh.shape["gx"] // CORES, mesh.shape["gy"])
    return jax.shard_map(
        functools.partial(body, dims),
        mesh=mesh,
        in_specs=in_specs,
        out_specs=P(tokens, None),
        check_vma=False,
    )
```

```python
import functools
import itertools
import math

import jax
import jax.numpy as jnp
from jax import lax
from jax.experimental import pallas as pl
from jax.experimental.pallas import tpu as pltpu
from jax.sharding import PartitionSpec as P

AXES = ("gx", "gy", "gz")
CORES = 2
MAX_RECEIVES = 256
STEP = 256
LUMPS = 8
VMEM_BYTES = 60 << 20
ORDERS = ((0, 1, 2), (1, 0, 2), (2, 0, 1), (2, 1, 0))
SHARES = (1, 1, 3, 3)


def rotate(values, positions):
    width = values.shape[-1]
    half = width // 2
    freqs = jnp.exp(-math.log(500000.0) * jnp.arange(half, dtype=jnp.float32) * 2.0 / width)
    angles = positions.astype(jnp.float32)[:, None] * freqs[None, :]
    cosine = jnp.concatenate([jnp.cos(angles), jnp.cos(angles)], -1)[:, None, :]
    sine = jnp.concatenate([jnp.sin(angles), jnp.sin(angles)], -1)[:, None, :]
    turned = jnp.concatenate([-values[..., half:], values[..., :half]], -1)
    return values * cosine + turned * sine


def attend(queries, keys, values, segment_ids, positions):
    count = queries.shape[0]
    scores = jnp.einsum(
        "thd,sd->hts", queries, keys, preferred_element_type=jnp.float32
    ) / math.sqrt(keys.shape[-1])
    allowed = (segment_ids[:, None] == segment_ids[None, :]) & (
        positions[None, :] <= positions[:, None]
    )
    scores = jnp.where(allowed[None], scores, -1e30)
    peak = jnp.max(scores, -1, keepdims=True)
    expd = jnp.exp(scores - peak)
    probs = (expd / jnp.sum(expd, -1, keepdims=True)).astype(jnp.bfloat16)
    mixed = jnp.einsum("hts,sd->thd", probs, values, preferred_element_type=jnp.float32)
    return mixed.astype(jnp.bfloat16).reshape(count, -1)


def arrivals(size):
    return [sorted(range(size), key=lambda other: (abs(other - own), other)) for own in range(size)]


def pick(table, place):
    if len(set(table)) == 1:
        return table[0]
    value = jnp.int32(table[0])
    for index in range(1, len(table)):
        value = jnp.where(place == index, jnp.int32(table[index]), value)
    return value


def pieces_of(rows, unit):
    units = rows // unit
    total = sum(SHARES)
    runs, start, seen = [], 0, 0
    for share in SHARES:
        seen += share
        stop = units * seen // total * unit
        runs.append((start, stop))
        start = stop
    return runs


def program_order(dims, pieces):
    events = []
    for number, (tensor, order, _) in enumerate(pieces):
        for combo in itertools.product(*(range(size) for size in dims)):
            hops, late = 0, 0
            for place, axis in enumerate(order):
                hops += combo[axis]
                late = late * 8 + combo[order[2 - place]]
            if hops:
                events.append((tensor, hops, late, number, combo))
    events.sort()
    return [(number, combo) for _, _, _, number, combo in events]


class Gather:
    def __init__(self, dims, pieces, refs_in, refs_out, slices, own_sems, send_sem, recv_sem, cross_sem):
        self.dims, self.pieces = dims, pieces
        self.refs_in, self.refs_out, self.slices = refs_in, refs_out, slices
        self.send_sem, self.recv_sem, self.cross_sem = send_sem, recv_sem, cross_sem
        gx, gy, gz = (lax.axis_index(name) for name in AXES)
        self.core = lax.rem(gx, CORES)
        self.me = (gz, lax.div(gx, CORES), gy)
        self.tables = [arrivals(size) for size in dims]
        self.sends = 0
        self.pending = []

    def device(self, place, core):
        x, y, z = place
        return (y * CORES + core, z, x)

    def line(self, place):
        x, y, z = place
        return (y * self.dims[2] + z) * self.dims[0] + x

    def block(self, place, core):
        x, y, z = place
        return ((y * CORES + core) * self.dims[2] + z) * self.dims[0] + x

    def neighbour(self, axis, step):
        place = list(self.me)
        place[axis] = place[axis] + step
        return tuple(place)

    def other(self, axis):
        place = list(self.me)
        place[axis] = 1 - place[axis]
        return tuple(place)

    def barrier(self):
        sem = pltpu.get_barrier_semaphore()
        mesh = pl.DeviceIdType.MESH
        count = 1
        pl.semaphore_signal(sem, inc=1, device_id=self.device(self.me, 1 - self.core), device_id_type=mesh)
        for axis, size in enumerate(self.dims):
            if size == 2:
                pl.semaphore_signal(
                    sem, inc=1, device_id=self.device(self.other(axis), self.core), device_id_type=mesh
                )
                count = count + 1
            elif size > 2:
                for step in (-1, 1):
                    inside = self.inside(axis, step)

                    @pl.when(inside)
                    def _(axis=axis, step=step):
                        pl.semaphore_signal(
                            sem,
                            inc=1,
                            device_id=self.device(self.neighbour(axis, step), self.core),
                            device_id_type=mesh,
                        )

                    count = count + inside.astype(jnp.int32)
        pl.semaphore_wait(sem, count)

    def inside(self, axis, step):
        return self.me[axis] > 0 if step < 0 else self.me[axis] < self.dims[axis] - 1

    def source(self, number, owner, own):
        tensor = self.pieces[number][0]
        if own:
            return self.slices[tensor](self.refs_in[tensor], None, self.pieces[number][2])
        return self.slices[tensor](self.refs_out[tensor], self.block(owner, self.core), self.pieces[number][2])

    def copy(self, number, owner, own, device, sem, cross=False):
        tensor = self.pieces[number][0]
        target = self.slices[tensor](self.refs_out[tensor], self.block(owner, self.core), self.pieces[number][2])
        landed = self.cross_sem if cross else self.recv_sem
        return pltpu.make_async_remote_copy(
            src_ref=self.source(number, owner, own),
            dst_ref=target,
            send_sem=self.send_sem.at[sem],
            recv_sem=landed.at[number, self.line(owner)],
            device_id=device,
            device_id_type=pl.DeviceIdType.MESH,
        )

    def send(self, number, owner, own, place, condition=None, cross=False):
        sem = self.sends
        self.sends += 1
        core = 1 - self.core if cross else self.core

        def make():
            return self.copy(number, owner, own, self.device(place, core), sem, cross)

        if condition is None:
            make().start()
        else:
            pl.when(condition)(lambda: make().start())
        self.pending.append((make, condition))

    def pass_on(self, number, combo):
        order = self.pieces[number][1]
        owner = tuple(
            pick([row[index] for row in table], here)
            for table, index, here in zip(self.tables, combo, self.me)
        )
        own = not any(combo)
        last = max((place for place, axis in enumerate(order) if combo[axis]), default=-1)
        if last >= 0:
            axis = order[last]
            if self.dims[axis] > 2:
                up = owner[axis] < self.me[axis]
                step = jnp.where(up, 1, -1)
                goes = jnp.where(up, self.me[axis] < self.dims[axis] - 1, self.me[axis] > 0)
                self.send(number, owner, own, self.neighbour(axis, step), goes)
        for axis in order[last + 1 :]:
            if self.dims[axis] == 2:
                self.send(number, owner, own, self.other(axis))
            elif self.dims[axis] > 2:
                for step in (-1, 1):
                    self.send(number, owner, own, self.neighbour(axis, step), self.inside(axis, step))
        self.send(number, owner, own, self.me, cross=True)

    def take(self, number, combo, cross=False):
        owner = tuple(
            pick([row[index] for row in table], here)
            for table, index, here in zip(self.tables, combo, self.me)
        )
        tensor = self.pieces[number][0]
        core = 1 - self.core if cross else self.core
        landed = self.slices[tensor](self.refs_out[tensor], self.block(owner, core), self.pieces[number][2])
        sem = self.cross_sem if cross else self.recv_sem
        pltpu.make_async_copy(landed, landed, sem.at[number, self.line(owner)]).wait()

    def drain(self):
        for make, condition in self.pending:
            if condition is None:
                make().wait_send()
            else:
                pl.when(condition)(lambda make=make: make().wait_send())


def project(x_ref, wf_ref, acc_ref, lump):
    steps = x_ref.shape[1] // STEP // LUMPS

    @pl.loop(0, steps)
    def _(index):
        span = pl.ds(pl.multiple_of((lump * steps + index) * STEP, STEP), STEP)
        acc_ref[...] += jnp.dot(x_ref[:, span], wf_ref[span, :], preferred_element_type=jnp.float32)


def attend_local(x_ref, acc_ref, cos_ref, sin_ref, mask_ref, mixed_ref):
    count, width = x_ref.shape
    size = cos_ref.shape[1]
    heads = mixed_ref.shape[1] // size

    def squares(index, total):
        part = x_ref[:, pl.ds(pl.multiple_of(index * STEP, STEP), STEP)].astype(jnp.float32)
        return total + jnp.sum(part * part, -1, keepdims=True)

    total = lax.fori_loop(0, width // STEP, squares, jnp.zeros((count, 1), jnp.float32))
    inverse = lax.rsqrt(total / width + 1e-05)
    cosine, sine = cos_ref[...], sin_ref[...]

    def turned(head):
        raw = acc_ref[:, head * size : (head + 1) * size] * inverse
        return (raw * cosine + pltpu.roll(raw, size // 2, 1) * sine).astype(jnp.bfloat16)

    keys = turned(heads)
    values = (acc_ref[:, (heads + 1) * size :] * inverse).astype(jnp.bfloat16)
    allowed = mask_ref[...] > 0.5
    for head in range(heads):
        scores = lax.dot_general(
            turned(head), keys, (((1,), (1,)), ((), ())), preferred_element_type=jnp.float32
        ) / math.sqrt(size)
        scores = jnp.where(allowed, scores, -1e30)
        expd = jnp.exp(scores - jnp.max(scores, -1, keepdims=True))
        probs = (expd / jnp.sum(expd, -1, keepdims=True)).astype(jnp.bfloat16)
        mixed = jnp.dot(probs, values, preferred_element_type=jnp.float32)
        mixed_ref[:, head * size : (head + 1) * size] = mixed.astype(jnp.bfloat16)


def gather_kernel(
    dims, pieces, order, w_ref, o_ref, stream_ref, cos_ref, sin_ref, mask_ref, mixed_ref, of_ref,
    wf_ref, x_ref, acc_ref, own_sem, send_sem, recv_sem, cross_sem,
):
    rows = w_ref.shape[0]
    cols = o_ref.shape[1]

    def w_slice(ref, block, run):
        start = run[0] if block is None else block * rows + run[0]
        if block is not None:
            start = pl.multiple_of(start, 16)
        return ref.at[pl.ds(start, run[1] - run[0]), :]

    def o_slice(ref, block, run):
        if block is None:
            return ref.at[pl.ds(run[0], run[1] - run[0]), :]
        return ref.at[pl.ds(run[0], run[1] - run[0]), pl.ds(pl.multiple_of(block * cols, cols), cols)]

    g = Gather(dims, pieces, (w_ref, o_ref), (wf_ref, of_ref), (w_slice, o_slice), own_sem, send_sem, recv_sem, cross_sem)
    mine = g.block(g.me, g.core)
    keep_w = pltpu.make_async_copy(w_ref, w_slice(wf_ref, mine, (0, rows)), own_sem.at[0])
    keep_o = pltpu.make_async_copy(o_ref, o_slice(of_ref, mine, (0, o_ref.shape[0])), own_sem.at[1])
    fetch = pltpu.make_async_copy(stream_ref, x_ref, own_sem.at[2])
    g.barrier()
    zero = (0, 0, 0)
    numbers = list(range(len(pieces)))
    for number in reversed(numbers):
        if pieces[number][0] == 0:
            g.pass_on(number, zero)
    keep_w.start()
    keep_o.start()
    fetch.start()
    acc_ref[...] = jnp.zeros_like(acc_ref)
    events = [(number, zero) for number in numbers] + list(order)
    weights = sum(1 for number, _ in order if pieces[number][0] == 0)
    gap = max((len(order) - weights) // (2 * LUMPS), 1)
    for index, (number, combo) in enumerate(order):
        if index == weights // 2:
            for later in reversed(numbers):
                if pieces[later][0] == 1:
                    g.pass_on(later, zero)
        g.take(number, combo)
        g.pass_on(number, combo)
        since = index - weights
        if since == gap:
            for event in events:
                if pieces[event[0]][0] == 0:
                    g.take(*event, cross=True)
            keep_w.wait()
            fetch.wait()
        if since >= gap and since % gap == 0 and since // gap <= LUMPS:
            project(x_ref, wf_ref, acc_ref, since // gap - 1)
        if since == gap * (LUMPS + 1):
            attend_local(x_ref, acc_ref, cos_ref, sin_ref, mask_ref, mixed_ref)
    for event in events:
        if pieces[event[0]][0] == 1:
            g.take(*event, cross=True)
    g.drain()
    keep_o.wait()


def count_sends(dims, pieces):
    total = 0
    for _, order, _ in pieces:
        for combo in itertools.product(*(range(size) for size in dims)):
            last = max((place for place, axis in enumerate(order) if combo[axis]), default=-1)
            if last >= 0 and dims[order[last]] > 2:
                total += 1
            total += sum(min(dims[axis] - 1, 2) for axis in order[last + 1 :]) + 1
    return total


def gather_all(dims, weight, out_weight, stream, cosine, sine, mask):
    rows, width = weight.shape
    depth, cols = out_weight.shape
    count = math.prod(dims) * CORES
    pieces = [(0, order, run) for order, run in zip(ORDERS, pieces_of(rows, 16))]
    pieces += [(1, order, run) for order, run in zip(ORDERS, pieces_of(depth, 16))]
    pieces = [piece for piece in pieces if piece[2][1] > piece[2][0]]
    order = program_order(dims, pieces)
    lines = math.prod(dims)
    return pl.pallas_call(
        functools.partial(gather_kernel, dims, pieces, order),
        out_shape=(
            jax.ShapeDtypeStruct((stream.shape[0], depth), stream.dtype),
            jax.ShapeDtypeStruct((depth, count * cols), out_weight.dtype),
        ),
        in_specs=[pl.BlockSpec(memory_space=pl.ANY)] * 3 + [pl.BlockSpec(memory_space=pltpu.VMEM)] * 3,
        out_specs=[pl.BlockSpec(memory_space=pltpu.VMEM), pl.BlockSpec(memory_space=pl.ANY)],
        scratch_shapes=[
            pltpu.VMEM((count * rows, width), weight.dtype),
            pltpu.VMEM(stream.shape, stream.dtype),
            pltpu.VMEM((stream.shape[0], width), jnp.float32),
            pltpu.SemaphoreType.DMA((3,)),
            pltpu.SemaphoreType.DMA((count_sends(dims, pieces),)),
            pltpu.SemaphoreType.DMA((len(pieces), lines)),
            pltpu.SemaphoreType.DMA((len(pieces), lines)),
        ],
        compiler_params=pltpu.CompilerParams(collective_id=0, has_side_effects=True, vmem_limit_bytes=VMEM_BYTES),
    )(weight, out_weight, stream, cosine, sine, mask)


def body(dims, stream, segment_ids, positions, norm_gain, q_weight, k_weight, v_weight, o_weight):
    count = stream.shape[0]
    head_size = k_weight.shape[2]
    queries_width = q_weight.shape[2]
    widened = stream.astype(jnp.float32)
    joined = jnp.concatenate([q_weight[0], k_weight[0], v_weight[0]], -1).astype(jnp.float32)
    weight = (joined * norm_gain[0].astype(jnp.float32)[:, None]).astype(jnp.bfloat16)
    if CORES * len(ORDERS) * math.prod(dims) <= MAX_RECEIVES:
        half = head_size // 2
        freqs = jnp.exp(-math.log(500000.0) * jnp.arange(half, dtype=jnp.float32) * 2.0 / head_size)
        angles = positions.astype(jnp.float32)[:, None] * freqs[None, :]
        cosine = jnp.concatenate([jnp.cos(angles), jnp.cos(angles)], -1)
        sine = jnp.concatenate([-jnp.sin(angles), jnp.sin(angles)], -1)
        allowed = (segment_ids[:, None] == segment_ids[None, :]) & (positions[None, :] <= positions[:, None])
        mixed, out_full = gather_all(
            dims, weight, o_weight[0], stream, cosine, sine, allowed.astype(jnp.float32)
        )
    else:
        full, out_full = weight, o_weight[0]
        for name in reversed(AXES):
            full = lax.all_gather(full, name, axis=0, tiled=True)
            out_full = lax.all_gather(out_full, name, axis=1, tiled=True)
        inverse = lax.rsqrt(jnp.mean(widened * widened, -1, keepdims=True) + 1e-05)
        raw = jnp.dot(stream, full, preferred_element_type=jnp.float32) * inverse
        query_raw = raw[:, :queries_width]
        key_raw = raw[:, queries_width : queries_width + head_size]
        value_raw = raw[:, queries_width + head_size :]
        queries = rotate(query_raw.reshape(count, -1, head_size), positions).astype(jnp.bfloat16)
        keys = rotate(key_raw[:, None, :], positions)[:, 0, :].astype(jnp.bfloat16)
        values = value_raw.astype(jnp.bfloat16)
        mixed = attend(queries, keys, values, segment_ids, positions)
    branch = jnp.dot(mixed, out_full, preferred_element_type=jnp.float32)
    return (widened + branch).astype(jnp.bfloat16)


def solution(mesh):
    tokens = AXES
    in_specs = (
        P(tokens, None),
        P(tokens),
        P(tokens),
        P(None, tokens),
        P(None, tokens, None),
        P(None, tokens, None),
        P(None, tokens, None),
        P(None, None, tokens),
    )
    dims = (mesh.shape["gz"], mesh.shape["gx"] // CORES, mesh.shape["gy"])
    return jax.shard_map(
        functools.partial(body, dims),
        mesh=mesh,
        in_specs=in_specs,
        out_specs=P(tokens, None),
        check_vma=False,
    )
```

```python
import functools
import itertools
import math

import jax
import jax.numpy as jnp
from jax import lax
from jax.experimental import pallas as pl
from jax.experimental.pallas import tpu as pltpu
from jax.sharding import PartitionSpec as P

AXES = ("gx", "gy", "gz")
CORES = 2
MAX_RECEIVES = 256
STEP = 256
LUMPS = 8
VMEM_BYTES = 60 << 20
ORDERS = ((0, 1, 2), (1, 0, 2), (2, 0, 1), (2, 1, 0))
SHARES = (1, 1, 4, 4)


def rotate(values, positions):
    width = values.shape[-1]
    half = width // 2
    freqs = jnp.exp(-math.log(500000.0) * jnp.arange(half, dtype=jnp.float32) * 2.0 / width)
    angles = positions.astype(jnp.float32)[:, None] * freqs[None, :]
    cosine = jnp.concatenate([jnp.cos(angles), jnp.cos(angles)], -1)[:, None, :]
    sine = jnp.concatenate([jnp.sin(angles), jnp.sin(angles)], -1)[:, None, :]
    turned = jnp.concatenate([-values[..., half:], values[..., :half]], -1)
    return values * cosine + turned * sine


def attend(queries, keys, values, segment_ids, positions):
    count = queries.shape[0]
    scores = jnp.einsum(
        "thd,sd->hts", queries, keys, preferred_element_type=jnp.float32
    ) / math.sqrt(keys.shape[-1])
    allowed = (segment_ids[:, None] == segment_ids[None, :]) & (
        positions[None, :] <= positions[:, None]
    )
    scores = jnp.where(allowed[None], scores, -1e30)
    peak = jnp.max(scores, -1, keepdims=True)
    expd = jnp.exp(scores - peak)
    probs = (expd / jnp.sum(expd, -1, keepdims=True)).astype(jnp.bfloat16)
    mixed = jnp.einsum("hts,sd->thd", probs, values, preferred_element_type=jnp.float32)
    return mixed.astype(jnp.bfloat16).reshape(count, -1)


def arrivals(size):
    return [sorted(range(size), key=lambda other: (abs(other - own), other)) for own in range(size)]


def pick(table, place):
    if len(set(table)) == 1:
        return table[0]
    value = jnp.int32(table[0])
    for index in range(1, len(table)):
        value = jnp.where(place == index, jnp.int32(table[index]), value)
    return value


def pieces_of(rows, unit):
    units = rows // unit
    total = sum(SHARES)
    runs, start, seen = [], 0, 0
    for share in SHARES:
        seen += share
        stop = units * seen // total * unit
        runs.append((start, stop))
        start = stop
    return runs


def program_order(dims, pieces):
    events = []
    for number, (tensor, order, _) in enumerate(pieces):
        for combo in itertools.product(*(range(size) for size in dims)):
            hops, late = 0, 0
            for place, axis in enumerate(order):
                hops += combo[axis]
                late = late * 8 + combo[order[2 - place]]
            if hops:
                events.append((tensor, hops, late, number, combo))
    events.sort()
    return [(number, combo) for _, _, _, number, combo in events]


class Gather:
    def __init__(self, dims, pieces, refs_in, refs_out, slices, own_sems, send_sem, recv_sem, cross_sem):
        self.dims, self.pieces = dims, pieces
        self.refs_in, self.refs_out, self.slices = refs_in, refs_out, slices
        self.send_sem, self.recv_sem, self.cross_sem = send_sem, recv_sem, cross_sem
        gx, gy, gz = (lax.axis_index(name) for name in AXES)
        self.core = lax.rem(gx, CORES)
        self.me = (gz, lax.div(gx, CORES), gy)
        self.tables = [arrivals(size) for size in dims]
        self.sends = 0
        self.pending = []

    def device(self, place, core):
        x, y, z = place
        return (y * CORES + core, z, x)

    def line(self, place):
        x, y, z = place
        return (y * self.dims[2] + z) * self.dims[0] + x

    def block(self, place, core):
        x, y, z = place
        return ((y * CORES + core) * self.dims[2] + z) * self.dims[0] + x

    def neighbour(self, axis, step):
        place = list(self.me)
        place[axis] = place[axis] + step
        return tuple(place)

    def other(self, axis):
        place = list(self.me)
        place[axis] = 1 - place[axis]
        return tuple(place)

    def barrier(self):
        sem = pltpu.get_barrier_semaphore()
        mesh = pl.DeviceIdType.MESH
        count = 1
        pl.semaphore_signal(sem, inc=1, device_id=self.device(self.me, 1 - self.core), device_id_type=mesh)
        for axis, size in enumerate(self.dims):
            if size == 2:
                pl.semaphore_signal(
                    sem, inc=1, device_id=self.device(self.other(axis), self.core), device_id_type=mesh
                )
                count = count + 1
            elif size > 2:
                for step in (-1, 1):
                    inside = self.inside(axis, step)

                    @pl.when(inside)
                    def _(axis=axis, step=step):
                        pl.semaphore_signal(
                            sem,
                            inc=1,
                            device_id=self.device(self.neighbour(axis, step), self.core),
                            device_id_type=mesh,
                        )

                    count = count + inside.astype(jnp.int32)
        pl.semaphore_wait(sem, count)

    def inside(self, axis, step):
        return self.me[axis] > 0 if step < 0 else self.me[axis] < self.dims[axis] - 1

    def source(self, number, owner, own):
        tensor = self.pieces[number][0]
        if own:
            return self.slices[tensor](self.refs_in[tensor], None, self.pieces[number][2])
        return self.slices[tensor](self.refs_out[tensor], self.block(owner, self.core), self.pieces[number][2])

    def copy(self, number, owner, own, device, sem, cross=False):
        tensor = self.pieces[number][0]
        target = self.slices[tensor](self.refs_out[tensor], self.block(owner, self.core), self.pieces[number][2])
        landed = self.cross_sem if cross else self.recv_sem
        return pltpu.make_async_remote_copy(
            src_ref=self.source(number, owner, own),
            dst_ref=target,
            send_sem=self.send_sem.at[sem],
            recv_sem=landed.at[number, self.line(owner)],
            device_id=device,
            device_id_type=pl.DeviceIdType.MESH,
        )

    def send(self, number, owner, own, place, condition=None, cross=False):
        sem = self.sends
        self.sends += 1
        core = 1 - self.core if cross else self.core

        def make():
            return self.copy(number, owner, own, self.device(place, core), sem, cross)

        if condition is None:
            make().start()
        else:
            pl.when(condition)(lambda: make().start())
        self.pending.append((make, condition))

    def pass_on(self, number, combo):
        order = self.pieces[number][1]
        owner = tuple(
            pick([row[index] for row in table], here)
            for table, index, here in zip(self.tables, combo, self.me)
        )
        own = not any(combo)
        last = max((place for place, axis in enumerate(order) if combo[axis]), default=-1)
        if last >= 0:
            axis = order[last]
            if self.dims[axis] > 2:
                up = owner[axis] < self.me[axis]
                step = jnp.where(up, 1, -1)
                goes = jnp.where(up, self.me[axis] < self.dims[axis] - 1, self.me[axis] > 0)
                self.send(number, owner, own, self.neighbour(axis, step), goes)
        for axis in order[last + 1 :]:
            if self.dims[axis] == 2:
                self.send(number, owner, own, self.other(axis))
            elif self.dims[axis] > 2:
                for step in (-1, 1):
                    self.send(number, owner, own, self.neighbour(axis, step), self.inside(axis, step))
        self.send(number, owner, own, self.me, cross=True)

    def take(self, number, combo, cross=False):
        owner = tuple(
            pick([row[index] for row in table], here)
            for table, index, here in zip(self.tables, combo, self.me)
        )
        tensor = self.pieces[number][0]
        core = 1 - self.core if cross else self.core
        landed = self.slices[tensor](self.refs_out[tensor], self.block(owner, core), self.pieces[number][2])
        sem = self.cross_sem if cross else self.recv_sem
        pltpu.make_async_copy(landed, landed, sem.at[number, self.line(owner)]).wait()

    def drain(self):
        for make, condition in self.pending:
            if condition is None:
                make().wait_send()
            else:
                pl.when(condition)(lambda make=make: make().wait_send())


def project(x_ref, wf_ref, acc_ref, lump):
    steps = x_ref.shape[1] // STEP // LUMPS

    @pl.loop(0, steps)
    def _(index):
        span = pl.ds(pl.multiple_of((lump * steps + index) * STEP, STEP), STEP)
        acc_ref[...] += jnp.dot(x_ref[:, span], wf_ref[span, :], preferred_element_type=jnp.float32)


def attend_local(x_ref, acc_ref, cos_ref, sin_ref, mask_ref, mixed_ref):
    count, width = x_ref.shape
    size = cos_ref.shape[1]
    heads = mixed_ref.shape[1] // size

    def squares(index, total):
        part = x_ref[:, pl.ds(pl.multiple_of(index * STEP, STEP), STEP)].astype(jnp.float32)
        return total + jnp.sum(part * part, -1, keepdims=True)

    total = lax.fori_loop(0, width // STEP, squares, jnp.zeros((count, 1), jnp.float32))
    inverse = lax.rsqrt(total / width + 1e-05)
    cosine, sine = cos_ref[...], sin_ref[...]

    def turned(head):
        raw = acc_ref[:, head * size : (head + 1) * size] * inverse
        return (raw * cosine + pltpu.roll(raw, size // 2, 1) * sine).astype(jnp.bfloat16)

    keys = turned(heads)
    values = (acc_ref[:, (heads + 1) * size :] * inverse).astype(jnp.bfloat16)
    allowed = mask_ref[...] > 0.5
    for head in range(heads):
        scores = lax.dot_general(
            turned(head), keys, (((1,), (1,)), ((), ())), preferred_element_type=jnp.float32
        ) / math.sqrt(size)
        scores = jnp.where(allowed, scores, -1e30)
        expd = jnp.exp(scores - jnp.max(scores, -1, keepdims=True))
        probs = (expd / jnp.sum(expd, -1, keepdims=True)).astype(jnp.bfloat16)
        mixed = jnp.dot(probs, values, preferred_element_type=jnp.float32)
        mixed_ref[:, head * size : (head + 1) * size] = mixed.astype(jnp.bfloat16)


def gather_kernel(
    dims, pieces, order, w_ref, o_ref, stream_ref, cos_ref, sin_ref, mask_ref, mixed_ref, of_ref,
    wf_ref, x_ref, acc_ref, own_sem, send_sem, recv_sem, cross_sem,
):
    rows = w_ref.shape[0]
    cols = o_ref.shape[1]

    def w_slice(ref, block, run):
        start = run[0] if block is None else block * rows + run[0]
        if block is not None:
            start = pl.multiple_of(start, 16)
        return ref.at[pl.ds(start, run[1] - run[0]), :]

    def o_slice(ref, block, run):
        if block is None:
            return ref.at[pl.ds(run[0], run[1] - run[0]), :]
        return ref.at[pl.ds(run[0], run[1] - run[0]), pl.ds(pl.multiple_of(block * cols, cols), cols)]

    g = Gather(dims, pieces, (w_ref, o_ref), (wf_ref, of_ref), (w_slice, o_slice), own_sem, send_sem, recv_sem, cross_sem)
    mine = g.block(g.me, g.core)
    keep_w = pltpu.make_async_copy(w_ref, w_slice(wf_ref, mine, (0, rows)), own_sem.at[0])
    keep_o = pltpu.make_async_copy(o_ref, o_slice(of_ref, mine, (0, o_ref.shape[0])), own_sem.at[1])
    fetch = pltpu.make_async_copy(stream_ref, x_ref, own_sem.at[2])
    g.barrier()
    zero = (0, 0, 0)
    numbers = list(range(len(pieces)))
    for number in reversed(numbers):
        if pieces[number][0] == 0:
            g.pass_on(number, zero)
    keep_w.start()
    keep_o.start()
    fetch.start()
    acc_ref[...] = jnp.zeros_like(acc_ref)
    events = [(number, zero) for number in numbers] + list(order)
    weights = sum(1 for number, _ in order if pieces[number][0] == 0)
    gap = max((len(order) - weights) // (2 * LUMPS), 1)
    for index, (number, combo) in enumerate(order):
        if index == weights * 4 // 5:
            for later in reversed(numbers):
                if pieces[later][0] == 1:
                    g.pass_on(later, zero)
        g.take(number, combo)
        g.pass_on(number, combo)
        since = index - weights
        if since == gap:
            for event in events:
                if pieces[event[0]][0] == 0:
                    g.take(*event, cross=True)
            keep_w.wait()
            fetch.wait()
        if since >= gap and since % gap == 0 and since // gap <= LUMPS:
            project(x_ref, wf_ref, acc_ref, since // gap - 1)
        if since == gap * (LUMPS + 1):
            attend_local(x_ref, acc_ref, cos_ref, sin_ref, mask_ref, mixed_ref)
    for event in events:
        if pieces[event[0]][0] == 1:
            g.take(*event, cross=True)
    g.drain()
    keep_o.wait()


def count_sends(dims, pieces):
    total = 0
    for _, order, _ in pieces:
        for combo in itertools.product(*(range(size) for size in dims)):
            last = max((place for place, axis in enumerate(order) if combo[axis]), default=-1)
            if last >= 0 and dims[order[last]] > 2:
                total += 1
            total += sum(min(dims[axis] - 1, 2) for axis in order[last + 1 :]) + 1
    return total


def gather_all(dims, weight, out_weight, stream, cosine, sine, mask):
    rows, width = weight.shape
    depth, cols = out_weight.shape
    count = math.prod(dims) * CORES
    pieces = [(0, order, run) for order, run in zip(ORDERS, pieces_of(rows, 16))]
    pieces += [(1, order, run) for order, run in zip(ORDERS, pieces_of(depth, 16))]
    pieces = [piece for piece in pieces if piece[2][1] > piece[2][0]]
    order = program_order(dims, pieces)
    lines = math.prod(dims)
    return pl.pallas_call(
        functools.partial(gather_kernel, dims, pieces, order),
        out_shape=(
            jax.ShapeDtypeStruct((stream.shape[0], depth), stream.dtype),
            jax.ShapeDtypeStruct((depth, count * cols), out_weight.dtype),
        ),
        in_specs=[pl.BlockSpec(memory_space=pl.ANY)] * 3 + [pl.BlockSpec(memory_space=pltpu.VMEM)] * 3,
        out_specs=[pl.BlockSpec(memory_space=pltpu.VMEM), pl.BlockSpec(memory_space=pl.ANY)],
        scratch_shapes=[
            pltpu.VMEM((count * rows, width), weight.dtype),
            pltpu.VMEM(stream.shape, stream.dtype),
            pltpu.VMEM((stream.shape[0], width), jnp.float32),
            pltpu.SemaphoreType.DMA((3,)),
            pltpu.SemaphoreType.DMA((count_sends(dims, pieces),)),
            pltpu.SemaphoreType.DMA((len(pieces), lines)),
            pltpu.SemaphoreType.DMA((len(pieces), lines)),
        ],
        compiler_params=pltpu.CompilerParams(collective_id=0, has_side_effects=True, vmem_limit_bytes=VMEM_BYTES),
    )(weight, out_weight, stream, cosine, sine, mask)


def body(dims, stream, segment_ids, positions, norm_gain, q_weight, k_weight, v_weight, o_weight):
    count = stream.shape[0]
    head_size = k_weight.shape[2]
    queries_width = q_weight.shape[2]
    widened = stream.astype(jnp.float32)
    joined = jnp.concatenate([q_weight[0], k_weight[0], v_weight[0]], -1).astype(jnp.float32)
    weight = (joined * norm_gain[0].astype(jnp.float32)[:, None]).astype(jnp.bfloat16)
    if CORES * len(ORDERS) * math.prod(dims) <= MAX_RECEIVES:
        half = head_size // 2
        freqs = jnp.exp(-math.log(500000.0) * jnp.arange(half, dtype=jnp.float32) * 2.0 / head_size)
        angles = positions.astype(jnp.float32)[:, None] * freqs[None, :]
        cosine = jnp.concatenate([jnp.cos(angles), jnp.cos(angles)], -1)
        sine = jnp.concatenate([-jnp.sin(angles), jnp.sin(angles)], -1)
        allowed = (segment_ids[:, None] == segment_ids[None, :]) & (positions[None, :] <= positions[:, None])
        mixed, out_full = gather_all(
            dims, weight, o_weight[0], stream, cosine, sine, allowed.astype(jnp.float32)
        )
    else:
        full, out_full = weight, o_weight[0]
        for name in reversed(AXES):
            full = lax.all_gather(full, name, axis=0, tiled=True)
            out_full = lax.all_gather(out_full, name, axis=1, tiled=True)
        inverse = lax.rsqrt(jnp.mean(widened * widened, -1, keepdims=True) + 1e-05)
        raw = jnp.dot(stream, full, preferred_element_type=jnp.float32) * inverse
        query_raw = raw[:, :queries_width]
        key_raw = raw[:, queries_width : queries_width + head_size]
        value_raw = raw[:, queries_width + head_size :]
        queries = rotate(query_raw.reshape(count, -1, head_size), positions).astype(jnp.bfloat16)
        keys = rotate(key_raw[:, None, :], positions)[:, 0, :].astype(jnp.bfloat16)
        values = value_raw.astype(jnp.bfloat16)
        mixed = attend(queries, keys, values, segment_ids, positions)
    branch = jnp.dot(mixed, out_full, preferred_element_type=jnp.float32)
    return (widened + branch).astype(jnp.bfloat16)


def solution(mesh):
    tokens = AXES
    in_specs = (
        P(tokens, None),
        P(tokens),
        P(tokens),
        P(None, tokens),
        P(None, tokens, None),
        P(None, tokens, None),
        P(None, tokens, None),
        P(None, None, tokens),
    )
    dims = (mesh.shape["gz"], mesh.shape["gx"] // CORES, mesh.shape["gy"])
    return jax.shard_map(
        functools.partial(body, dims),
        mesh=mesh,
        in_specs=in_specs,
        out_specs=P(tokens, None),
        check_vma=False,
    )
```
